32 devices in a mesh: groups: 2 (over y), seq: 4 (over z), tp: 4 (over x, core).
Axes of the slice: x: 2, y: 2, z: 4, core: 2. Of those that a mesh axis runs over, the one named last changes fastest.
Arguments:
- q_prefill: bfloat16 [2048, 4096], P(('groups', 'seq'), 'tp'), parts along dimension 0, may hold values from -8 to 8
- k_prefill: bfloat16 [2048, 1024], P(('groups', 'seq'), 'tp'), parts along dimension 0, may hold values from -8 to 8
- v_prefill: bfloat16 [2048, 1024], P(('groups', 'seq'), 'tp'), parts along dimension 0, may hold values from -6 to 6
- pair_lengths: int32 [16], P('groups'), parts along dimension 0, may hold values from 1 to 640, 1024 in all
- q_decode: bfloat16 [8, 4096], P('groups', 'tp'), parts along dimension 0, may hold values from -8 to 8
- cache_k: bfloat16 [8, 256, 1024], P('groups', 'seq', 'tp'), parts along dimension 0, may hold values from -8 to 8
- cache_v: bfloat16 [8, 256, 1024], P('groups', 'seq', 'tp'), parts along dimension 0, may hold values from -6 to 6
- cache_lengths: int32 [8], P('groups'), parts along dimension 0, may hold values from 32 to 256
- stream: bfloat16 [24, 8192], P('groups', 'seq'), parts along dimension 0, may hold values from -40 to 40
- out_weight: bfloat16 [4096, 8192], P('tp', 'seq'), may hold values from -0.09375 to 0.09375
- norm_gain: bfloat16 [8192], P('seq'), may hold values from 0.099609375 to 1.8984375
- vocab_table: bfloat16 [64128, 8192], P('tp', 'seq'), may hold values from -0.0625 to 0.0625
- verdict_ids: int32 [24, 2], P('groups'), parts along dimension 0, may hold values from 0 to 64127
Outputs:
- attended: bfloat16 [2048, 4096], P(('groups', 'seq'), 'tp'), parts along dimension 0
- verdict_hidden: bfloat16 [24, 8192], P('groups', 'seq'), parts along dimension 0
- win: float32 [24], P('groups'), parts along dimension 0
The draws below stay inside these ranges and needn't reach their ends.
There are 2 independent parts, one for each index of `groups`. The reference program is written for one: setup_inputs(seed, part) draws one part's arguments, and reference() takes and returns one part's arrays. A program takes and returns all parts, laid end to end along the dimension named above; an argument that names none is the same for every part. Nothing has to cross between parts.
Inputs may be any that keep to these rules, and one draw needn't show every extreme that they name: `pair_lengths`: the segments lie end to end from position 0 and each is at most 640 long.
All inputs are finite; a program needn't handle non-finite values.
Results may differ from the reference program's by a relative error of at most 0.008.
Values may be sent and summed in bfloat16 or wider, within the bound.
A program may use at most 128 MiB of HBM per device.

```python
import math
import jax
import jax.numpy as jnp
import numpy as np
from jax import lax

D = 8192
H = 32
KVH = 8
HD = 128
VOCAB = 64128
TOK_DEV = 256
PAIRS = 8
PROMPTS = 4
STRETCH = 1024
MOST = 640
CACHE = 256
ROWS = 12


def base_field(key, shape):
    return jnp.clip(1.75 * jax.random.normal(key, shape, jnp.float32), -8.0, 8.0)


def marked_pair(sign_table, amplitudes):
    vectors = sign_table * amplitudes[:, None]
    shrink = 2.0 * math.sqrt(HD) / amplitudes
    second = vectors.at[:, 0].set(sign_table[:, 0] * (amplitudes - shrink))
    return (vectors, second)


def prefill_marks(key):
    base = jax.random.fold_in(key, 7001)
    key_pos, key_head, key_sign = jax.random.split(base, 3)
    positions = jax.random.randint(key_pos, (3,), 1, STRETCH)
    head_picks = jax.random.randint(key_head, (3,), 0, H)
    sign_table = (2 * jax.random.randint(key_sign, (3, HD), 0, 2) - 1).astype(jnp.float32)
    vectors, second = marked_pair(sign_table, jnp.array([7.5, 7.0, 6.5], jnp.float32))
    return (positions, head_picks, vectors, second)


def decode_marks(key):
    base = jax.random.fold_in(key, 7002)
    key_head, key_sign = jax.random.split(base, 2)
    head_picks = jax.random.randint(key_head, (PROMPTS,), 0, H)
    sign_table = (2 * jax.random.randint(key_sign, (PROMPTS, HD), 0, 2) - 1).astype(jnp.float32)
    amplitudes = jnp.array([7.5, 7.0, 6.5], jnp.float32)[jnp.arange(PROMPTS) % 3]
    vectors, second = marked_pair(sign_table, amplitudes)
    return (head_picks, vectors, second)


def draw_q_prefill(key, part):
    field = base_field(jax.random.fold_in(key, 1), (STRETCH, H * HD))
    positions, head_picks, vectors, second = prefill_marks(key)
    columns = head_picks[:, None] * HD + jnp.arange(HD)[None, :]
    field = field.at[positions[:, None], columns].set(vectors)
    return field.astype(jnp.bfloat16)


def draw_k_prefill(key, part):
    field = base_field(jax.random.fold_in(key, 2), (STRETCH, KVH * HD))
    positions, head_picks, vectors, second = prefill_marks(key)
    columns = (head_picks // (H // KVH))[:, None] * HD + jnp.arange(HD)[None, :]
    field = field.at[positions[:, None], columns].set(vectors)
    field = field.at[positions[:, None] - 1, columns].set(second)
    return field.astype(jnp.bfloat16)


def draw_q_decode(key, part):
    field = base_field(jax.random.fold_in(key, 3), (PROMPTS, H * HD))
    head_picks, vectors, second = decode_marks(key)
    columns = head_picks[:, None] * HD + jnp.arange(HD)[None, :]
    prompt_rows = jnp.arange(PROMPTS)[:, None]
    field = field.at[prompt_rows, columns].set(vectors)
    return field.astype(jnp.bfloat16)


def draw_cache_k(key, part):
    field = base_field(jax.random.fold_in(key, 4), (PROMPTS, CACHE, KVH * HD))
    head_picks, vectors, second = decode_marks(key)
    columns = (head_picks // (H // KVH))[:, None] * HD + jnp.arange(HD)[None, :]
    prompt_rows = jnp.arange(PROMPTS)[:, None]
    field = field.at[prompt_rows, 0, columns].set(vectors)
    field = field.at[prompt_rows, 1, columns].set(second)
    return field.astype(jnp.bfloat16)


def draw_stream(key, part):
    key_rows, key_noise = jax.random.split(jax.random.fold_in(key, 5), 2)
    row_scale = jnp.exp(jax.random.uniform(key_rows, (ROWS, 1), jnp.float32, math.log(0.3), math.log(3.0)))
    column_ramp = jnp.arange(D, dtype=jnp.float32)[None, :] / D
    noise_part = jnp.clip(jax.random.normal(key_noise, (ROWS, D), jnp.float32), -6.0, 6.0)
    column_scale = math.sqrt(3.0) ** column_ramp
    return (noise_part * row_scale * column_scale).astype(jnp.bfloat16)


def set_ends(drawn, key, low, high):
    longest = drawn.shape.index(max(drawn.shape))
    spots = []
    for shift in (0, 1):
        where = [jax.random.randint(jax.random.fold_in(key, axis), (), 0, length) for axis, length in enumerate(drawn.shape)]
        where[longest] = (where[longest] + shift) % drawn.shape[longest]
        spots.append(tuple(where))
    return drawn.at[spots[0]].set(low).at[spots[1]].set(high)


def shard_levels(stream_key, extent, pieces, least, high):
    factor_of, own = 1.0, jax.random.fold_in(stream_key, 6)
    for axis_at, blocks in pieces:
        steps = jnp.exp(jax.random.uniform(jax.random.fold_in(own, axis_at), (blocks,), jnp.float32, least / len(pieces), high / len(pieces)))
        factor_of = factor_of * jnp.repeat(steps, extent[axis_at] // blocks).reshape([-1 if axis == axis_at else 1 for axis in range(len(extent))])
    return factor_of


def length_profile(amount, total, most, lean):
    portions = [(1 << 20) // math.isqrt(standing ** lean) + 1 for standing in range(2, amount + 1)]
    spare, counts = total - most - (amount - 1), [1] * (amount - 1)
    while spare > 0:
        free = [i for i in range(amount - 1) if counts[i] < most]
        pool, budget = sum([portions[i] for i in free]), spare
        for i in free:
            more = min(most - counts[i], max(1, budget * portions[i] // pool), spare)
            counts[i] = counts[i] + more
            spare = spare - more
    return np.array([most] + counts)


def ragged_sizes(rng, amount, total, bound, slope):
    if amount == 2:
        one = jax.random.randint(rng, (), max(1, total - bound), min(bound, total - 1) + 1)
        return jnp.stack([one, total - one])
    lengths = jnp.asarray(length_profile(amount, total, bound, slope), jnp.int32)
    twos = (amount - 1) // 2
    giver, taker = lengths[1:1 + 2 * twos:2], lengths[2:2 + 2 * twos:2]
    slack = jnp.minimum(giver - 1, bound - taker)
    moved = jax.random.randint(jax.random.fold_in(rng, 1), (twos,), 0, 1 << 20) % (slack + 1)
    lengths = lengths.at[1:1 + 2 * twos:2].set(giver - moved).at[2:2 + 2 * twos:2].set(taker + moved)
    return lengths[jax.random.permutation(jax.random.fold_in(rng, 2), amount)]


def gaussian(rng, extent, scale, limit, cuts=(), held_as=jnp.bfloat16):
    loudness = shard_levels(rng, extent, cuts, -0.22, 0.18) if cuts else 1.0
    values = jax.random.normal(rng, extent, jnp.float32) * scale * loudness
    return jnp.minimum(jnp.maximum(values, -limit), limit).astype(held_as)


def setup_inputs(seed: int = 0, part: int = 0) -> dict:
    seeds = jax.random.split(jax.random.key(seed), 14)
    part_keys = jax.random.split(jax.random.fold_in(seeds[13], part), 14)
    return {
        "q_prefill": draw_q_prefill(jax.random.fold_in(jax.random.fold_in(seeds[13], part), 71), part),
        "k_prefill": draw_k_prefill(jax.random.fold_in(jax.random.fold_in(seeds[13], part), 71), part),
        "v_prefill": gaussian(part_keys[2], (STRETCH, KVH * HD), 1.0, 6.0, ((0, 4), (1, 4))),
        "pair_lengths": ragged_sizes(part_keys[3], PAIRS, STRETCH, MOST, 2).astype(jnp.int32),
        "q_decode": draw_q_decode(jax.random.fold_in(jax.random.fold_in(seeds[13], part), 71), part),
        "cache_k": draw_cache_k(jax.random.fold_in(jax.random.fold_in(seeds[13], part), 71), part),
        "cache_v": gaussian(part_keys[6], (PROMPTS, CACHE, KVH * HD), 1.0, 6.0, ((1, 4), (2, 4))),
        "cache_lengths": set_ends(jax.random.randint(part_keys[7], (PROMPTS,), CACHE // 8, CACHE + 1), jax.random.fold_in(part_keys[7], 1), CACHE // 8, CACHE).astype(jnp.int32),
        "stream": draw_stream(jax.random.fold_in(jax.random.fold_in(seeds[13], part), 71), part),
        "out_weight": gaussian(seeds[9], (H * HD, D), (H * HD) ** -0.5, 0.09375, ((0, 4), (1, 4))),
        "norm_gain": jnp.clip(1.0 + 0.18 * jax.random.normal(seeds[10], (D,), jnp.float32), 0.099609375, 1.8984375).astype(jnp.bfloat16),
        "vocab_table": gaussian(seeds[11], (VOCAB, D), D ** -0.5, 0.0625, ((0, 4), (1, 4))),
        "verdict_ids": set_ends(jax.random.randint(part_keys[12], (ROWS, 2), 0, VOCAB), jax.random.fold_in(part_keys[12], 1), 0, VOCAB - 1).astype(jnp.int32),
    }


masked_score = -1e+30
norm_eps = 1e-05

def segment_of(positions, pair_ends):
    return lax.optimization_barrier(jnp.sum((pair_ends[None, :] <= positions[:, None]).astype(jnp.int32), axis=1))

def reference(q_prefill, k_prefill, v_prefill, pair_lengths, q_decode, cache_k, cache_v, cache_lengths, stream, out_weight, norm_gain, vocab_table, verdict_ids):
    group_size = H // KVH
    score_scale = 1.0 / HD ** 0.5
    pair_ends = jnp.cumsum(pair_lengths).astype(jnp.int32)
    all_pos = jnp.arange(STRETCH, dtype=jnp.int32)
    all_seg = segment_of(all_pos, pair_ends)
    keys_all = k_prefill.reshape(STRETCH, KVH, HD).astype(jnp.float32)
    values_all = v_prefill.reshape(STRETCH, KVH, HD).astype(jnp.float32)

    def block(first_row):
        query_rows = lax.dynamic_slice_in_dim(q_prefill, first_row, TOK_DEV, 0)
        query_rows = query_rows.reshape(TOK_DEV, KVH, group_size, HD).astype(jnp.float32)
        query_pos = first_row + jnp.arange(TOK_DEV, dtype=jnp.int32)
        query_seg = lax.dynamic_slice_in_dim(all_seg, first_row, TOK_DEV, 0)
        scores = jnp.einsum('qkgd,nkd->kgqn', query_rows, keys_all) * score_scale
        visible = (query_seg[:, None] == all_seg[None, :]) & (all_pos[None, :] <= query_pos[:, None])
        scores = jnp.where(visible, scores, masked_score)
        row_max = lax.optimization_barrier(jnp.max(scores, axis=-1, keepdims=True))
        exp_terms = jnp.where(visible, jnp.exp(scores - row_max), 0.0)
        row_total = lax.optimization_barrier(jnp.sum(exp_terms, axis=-1))
        weights = exp_terms.astype(jnp.bfloat16).astype(jnp.float32)
        summed = jnp.einsum('kgqn,nkd->kgqd', weights, values_all) / row_total[..., None]
        return jnp.transpose(summed, (2, 0, 1, 3)).reshape(TOK_DEV, H * HD).astype(jnp.bfloat16)
    starts = jnp.arange(0, STRETCH, TOK_DEV, dtype=jnp.int32)
    attended = lax.map(block, starts).reshape(STRETCH, H * HD)
    dec_queries = q_decode.reshape(PROMPTS, KVH, group_size, HD).astype(jnp.float32)
    dec_keys = cache_k.reshape(PROMPTS, CACHE, KVH, HD).astype(jnp.float32)
    dec_values = cache_v.reshape(PROMPTS, CACHE, KVH, HD).astype(jnp.float32)
    dec_scores = jnp.einsum('pkgd,pckd->pkgc', dec_queries, dec_keys) * score_scale
    valid = (jnp.arange(CACHE, dtype=jnp.int32)[None, :] < cache_lengths[:, None])[:, None, None, :]
    dec_scores = jnp.where(valid, dec_scores, masked_score)
    dec_max = lax.optimization_barrier(jnp.max(dec_scores, axis=-1, keepdims=True))
    dec_exp = jnp.where(valid, jnp.exp(dec_scores - dec_max), 0.0)
    dec_total = lax.optimization_barrier(jnp.sum(dec_exp, axis=-1))
    dec_weights = dec_exp.astype(jnp.bfloat16).astype(jnp.float32)
    decode_out = jnp.einsum('pkgc,pckd->pkgd', dec_weights, dec_values) / dec_total[..., None]
    decode_out = decode_out.reshape(PROMPTS, H * HD).astype(jnp.bfloat16)
    verdict_in = jnp.concatenate([attended[pair_ends - 1], decode_out], axis=0)
    residual = stream.astype(jnp.float32) + jnp.dot(verdict_in, out_weight, preferred_element_type=jnp.float32)
    inv_rms = 1.0 / jnp.sqrt(lax.optimization_barrier(jnp.mean(residual * residual, axis=1)) + norm_eps)
    gained = residual * norm_gain.astype(jnp.float32)[None, :]
    verdict_hidden = (gained * inv_rms[:, None]).astype(jnp.bfloat16)
    table_rows = vocab_table[verdict_ids].astype(jnp.float32)
    verdict_logits = inv_rms[:, None] * lax.optimization_barrier(jnp.sum(gained[:, None, :] * table_rows, axis=2))
    win = 1.0 / (1.0 + jnp.exp(verdict_logits[:, 1] - verdict_logits[:, 0]))
    return (attended, verdict_hidden, win)
```

```python
import functools
import math

import jax
import jax.numpy as jnp
from jax import lax
from jax.experimental import pallas as pl
from jax.experimental.pallas import tpu as pltpu
from jax.sharding import PartitionSpec as P

HD = 128
ROW = 8
MASKED = -1e30
EPS = 1e-05
BF = jnp.bfloat16
F32 = jnp.float32
MESH = pl.DeviceIdType.MESH


def up(value, step):
    return -(-value // step) * step


def dot(a, b, dims):
    return lax.dot_general(a, b, (dims, ((), ())), preferred_element_type=F32)


def kernel(
    ns, nt, width, spans,
    len_ref, clen_ref, q_ref, k_ref, v_ref, qd_ref, ck_ref, cv_ref, stream_ref, gain_ref, tbl_ref, w_ref,
    att_ref, hid_ref, win_ref,
    kbuf, vbuf, bias, mrow, lrow, acc, qdpad, qsel, qx, pout, pstat, pox, psx, wbuf, part, partx, tblx, stat, statx,
    ks, kr, vs, vr, qs, qr, pos, por, pss, psr, ts, tr, gs, gr, ss, sr, wsem,
):
    me = lax.axis_index("seq")
    mt = lax.axis_index("tp")
    tokens = q_ref.shape[0]
    heads = q_ref.shape[1] // HD
    kvl = k_ref.shape[1] // HD
    group = heads // kvl
    pairs = len_ref.shape[0]
    prompts, cache_n = ck_ref.shape[0], ck_ref.shape[1]
    scale2 = math.log2(math.e) / HD**0.5
    reach = len(spans)
    cols = pstat.shape[1]

    def head(h):
        return slice(h * HD, (h + 1) * HD)

    def relay(d, keys):
        src, buf, send, recv = (k_ref, kbuf, ks, kr) if keys else (v_ref, vbuf, vs, vr)
        low = spans[d - 1]
        rows = pl.ds(low, tokens - low)
        block = src.at[rows] if d == 1 else buf.at[d - 2, rows]
        return pltpu.make_async_remote_copy(
            src_ref=block,
            dst_ref=buf.at[d - 1, rows],
            send_sem=send.at[d - 1],
            recv_sem=recv.at[d - 1],
            device_id={"seq": lax.rem(me + 1, ns)},
            device_id_type=MESH,
        )

    def sends(d):
        return (me < ns - 1) & (me >= d - 1)

    def exchange(src, dst, send, recv, axis, mine, count):
        return [
            pltpu.make_async_remote_copy(
                src_ref=src,
                dst_ref=dst.at[mine],
                send_sem=send.at[d - 1],
                recv_sem=recv.at[d - 1],
                device_id={axis: lax.rem(mine + d, count)},
                device_id_type=MESH,
            )
            for d in range(1, count)
        ]

    weight_copy = pltpu.make_async_copy(w_ref, wbuf, wsem)
    weight_copy.start()
    barrier = pltpu.get_barrier_semaphore()
    for d in range(1, ns):
        pl.semaphore_signal(barrier, inc=1, device_id={"seq": lax.rem(me + d, ns)}, device_id_type=MESH)
    for d in range(1, nt):
        pl.semaphore_signal(barrier, inc=1, device_id={"tp": lax.rem(mt + d, nt)}, device_id_type=MESH)

    ends, total = [], jnp.int32(0)
    for p in range(pairs):
        total = total + len_ref[p]
        ends.append(total)
    starts = [jnp.int32(0)] + ends[:-1]
    first = me * tokens
    row_p = lax.broadcasted_iota(jnp.int32, (ROW, tokens), 0)
    last = jnp.full((ROW, tokens), -1, jnp.int32)
    for p in range(pairs):
        last = jnp.where(row_p == p, ends[p] - 1 - first, last)
    chosen = (lax.broadcasted_iota(jnp.int32, (ROW, tokens), 1) == last).astype(F32).astype(BF)
    picked = dot(chosen, q_ref[...], ((1,), (0,)))
    qsel[...] = picked.astype(BF)

    if ns + nt > 2:
        pl.semaphore_wait(barrier, ns + nt - 2)
    if reach:
        @pl.when(sends(1))
        def _():
            relay(1, True).start()

    q_moves = exchange(qsel, qx, qs, qr, "seq", me, ns)
    for move in q_moves:
        move.start()
    if reach:
        @pl.when(sends(1))
        def _():
            relay(1, False).start()

    t_moves = exchange(tbl_ref, tblx, gs, gr, "tp", mt, nt)
    for move in t_moves:
        move.start()

    q_pos = lax.broadcasted_iota(jnp.int32, (tokens, tokens), 1)
    k_pos = lax.broadcasted_iota(jnp.int32, (tokens, tokens), 0)
    seg_start = jnp.zeros((1, tokens), jnp.int32)
    q_row = lax.broadcasted_iota(jnp.int32, (1, tokens), 1) + first
    for p in range(pairs):
        seg_start = jnp.where(ends[p] <= q_row, ends[p], seg_start)
    seg_local = seg_start - first

    def attend(d, low):
        count = tokens - low
        if d == 0:
            visible = (k_pos >= seg_local) & (k_pos <= q_pos)
        else:
            visible = k_pos[:count] + (low - d * tokens) >= seg_local
        bias[:count, :] = jnp.where(visible, 0.0, MASKED)
        for kv in range(kvl):
            if d == 0:
                keys, values = k_ref[:, head(kv)], v_ref[:, head(kv)]
            else:
                keys, values = kbuf[d - 1, low:, head(kv)], vbuf[d - 1, low:, head(kv)]
            values_t = values.T
            for g in range(group):
                h = kv * group + g
                s = dot(keys, q_ref[:, head(h)], ((1,), (1,))) + bias[:count, :]
                top = jnp.max(s, axis=0, keepdims=True)
                if d:
                    old = mrow[h : h + 1, :]
                    top = jnp.maximum(top, old)
                p = jnp.exp2((s - top) * scale2)
                weighted = dot(values_t, p.astype(BF), ((1,), (0,)))
                summed = jnp.sum(p, axis=0, keepdims=True)
                if d:
                    keep = jnp.exp2((old - top) * scale2)
                    summed = summed + lrow[h : h + 1, :] * keep
                    weighted = weighted + acc[h] * keep
                mrow[h : h + 1, :] = top
                lrow[h : h + 1, :] = summed
                acc[h] = weighted

    def step(d):
        @pl.when(me >= d)
        def _():
            relay(d, True).wait_recv()
            if d < reach:
                @pl.when(sends(d + 1))
                def _():
                    relay(d + 1, True).start()
            relay(d, False).wait_recv()
            if d < reach:
                @pl.when(sends(d + 1))
                def _():
                    relay(d + 1, False).start()
            attend(d, spans[d - 1])

    attend(0, 0)

    for move in q_moves:
        move.wait_recv()
    q_pair = qsel[...].astype(F32)
    for d in range(1, ns):
        q_pair = q_pair + qx[lax.rem(me + d, ns)].astype(F32)
    qdpad[...] = jnp.zeros_like(qdpad)
    qdpad[:prompts, :] = qd_ref[...].astype(F32)
    q_dec = qdpad[...]
    pieces = [side[:, head(h)] for side in (q_pair, q_dec) for h in range(heads)]
    used = 2 * heads * ROW
    if cols > used:
        pieces.append(jnp.zeros((cols - used, HD), F32))
    q_cols = jnp.concatenate(pieces, axis=0).astype(BF)

    col = lax.broadcasted_iota(jnp.int32, (1, cols), 1)
    col_row = lax.rem(col, ROW)
    low_pair, high_pair = jnp.zeros((1, cols), jnp.int32), jnp.zeros((1, cols), jnp.int32)
    low_dec, high_dec = low_pair, high_pair
    for p in range(pairs):
        low_pair = jnp.where(col_row == p, starts[p] - first, low_pair)
        high_pair = jnp.where(col_row == p, ends[p] - first, high_pair)
    for p in range(prompts):
        ours = jnp.minimum(jnp.maximum(clen_ref[p] - me * cache_n, 0), cache_n)
        low_dec = jnp.where(col_row == p, p * cache_n, low_dec)
        high_dec = jnp.where(col_row == p, p * cache_n + ours, high_dec)

    blocks = []
    for kind in range(2):
        for kv in range(kvl):
            if kind == 0:
                keys, values = k_ref[:, head(kv)], v_ref[:, head(kv)]
                low_j, high_j = low_pair, high_pair
            else:
                keys = ck_ref[:, :, head(kv)].reshape(prompts * cache_n, HD)
                values = cv_ref[:, :, head(kv)].reshape(prompts * cache_n, HD)
                low_j, high_j = low_dec, high_dec
            begin = (kind * heads + kv * group) * ROW
            inside = (col >= begin) & (col < begin + group * ROW)
            high_j = jnp.where(inside, high_j, low_j)
            index = lax.broadcasted_iota(jnp.int32, (keys.shape[0], cols), 0)
            visible = (index >= low_j) & (index < high_j)
            s = jnp.where(visible, dot(keys, q_cols, ((1,), (1,))), MASKED)
            blocks.append((visible, s, values))
    top = functools.reduce(jnp.maximum, [jnp.max(s, axis=0, keepdims=True) for _, s, _ in blocks])
    p_sum = jnp.zeros((1, cols), F32)
    p_out = jnp.zeros((HD, cols), F32)
    for visible, s, values in blocks:
        p = jnp.where(visible, jnp.exp2((s - top) * scale2), 0.0)
        p_sum = p_sum + jnp.sum(p, axis=0, keepdims=True)
        p_out = p_out + dot(values.T, p.astype(BF), ((1,), (0,)))
    pout[...] = p_out.astype(BF)
    stat_row = lax.broadcasted_iota(jnp.int32, (ROW, cols), 0)
    pstat[...] = jnp.where(stat_row == 0, top, p_sum)
    o_moves = exchange(pout, pox, pos, por, "seq", me, ns)
    s_moves = exchange(pstat, psx, pss, psr, "seq", me, ns)
    for move, other in zip(o_moves, s_moves):
        move.start()
        other.start()
    pox[me] = pout[...]
    psx[me] = pstat[...]

    if reach:
        step(1)

    for move, other in zip(o_moves, s_moves):
        move.wait_recv()
        other.wait_recv()
    top = psx[0, 0:1, :]
    for i in range(1, ns):
        top = jnp.maximum(top, psx[i, 0:1, :])
    p_sum = jnp.zeros((1, cols), F32)
    p_out = jnp.zeros((HD, cols), F32)
    for i in range(ns):
        keep = jnp.exp2((psx[i, 0:1, :] - top) * scale2)
        p_sum = p_sum + psx[i, 1:2, :] * keep
        p_out = p_out + pox[i].astype(F32) * keep
    rows_t = (p_out / jnp.where(p_sum > 0.0, p_sum, 1.0)).T
    sides = [
        jnp.concatenate([rows_t[(kind * heads + h) * ROW : (kind * heads + h + 1) * ROW, :] for h in range(heads)], axis=1)
        for kind in range(2)
    ]
    verdict_in = jnp.concatenate(sides, axis=0).astype(BF)
    weight_copy.wait()
    part[...] = dot(verdict_in, wbuf[...], ((1,), (0,))).astype(BF)
    a_moves = exchange(part, partx, ts, tr, "tp", mt, nt)
    for move in a_moves:
        move.start()
    partx[mt] = part[...]
    tblx[mt] = tbl_ref[...]

    if reach > 1:
        step(2)

    for move in t_moves + a_moves:
        move.wait_recv()
    rows = stream_ref.shape[0]
    table = tblx[0].astype(F32)
    added = partx[0].astype(F32)
    for i in range(1, nt):
        table = table + tblx[i].astype(F32)
        added = added + partx[i].astype(F32)
    half = table.shape[0] // 2
    residual = stream_ref[...].astype(F32) + jnp.concatenate([added[:pairs], added[ROW : ROW + prompts]], axis=0)
    gained = residual * gain_ref[...].astype(F32)
    squares = jnp.sum(residual * residual, axis=1, keepdims=True)
    raw0 = jnp.sum(gained * table[:rows], axis=1, keepdims=True)
    raw1 = jnp.sum(gained * table[half : half + rows], axis=1, keepdims=True)
    lane = lax.broadcasted_iota(jnp.int32, stat.shape, 1)
    stat[...] = jnp.where(lane == 0, squares, jnp.where(lane == 1, raw0, raw1))
    f_moves = exchange(stat, statx, ss, sr, "seq", me, ns)
    for move in f_moves:
        move.start()
    statx[me] = stat[...]

    for d in range(3, reach + 1):
        step(d)

    for h in range(heads):
        att_ref[:, head(h)] = (acc[h] / lrow[h : h + 1, :]).T.astype(BF)

    for move in f_moves:
        move.wait_recv()
    sums = statx[0]
    for i in range(1, ns):
        sums = sums + statx[i]
    inv = 1.0 / jnp.sqrt(sums[:, 0:1] / width + EPS)
    hid_ref[...] = (gained * inv).astype(BF)
    win = 1.0 / (1.0 + jnp.exp(sums[:, 2:3] * inv - sums[:, 1:2] * inv))
    win_ref[...] = jnp.broadcast_to(win, win_ref.shape)

    for d in range(1, reach + 1):
        @pl.when(sends(d))
        def _():
            relay(d, True).wait_send()
            relay(d, False).wait_send()
    for move in q_moves + t_moves + o_moves + s_moves + a_moves + f_moves:
        move.wait_send()


def shards(
    ns, nt, width,
    q_prefill, k_prefill, v_prefill, pair_lengths, q_decode, cache_k, cache_v, cache_lengths,
    stream, out_weight, norm_gain, vocab_table, verdict_ids,
):
    tokens, kv_width = k_prefill.shape
    heads = q_prefill.shape[1] // HD
    rows, columns = stream.shape
    most = tokens * ns * 5 // 8
    spans = []
    for d in range(1, ns):
        low = max(0, d * tokens - most + 1)
        if low < tokens:
            spans.append(low // 128 * 128)
    reach = len(spans)
    slots = max(reach, 1)
    cols = up(2 * heads * ROW, 128)
    half = up(rows, 16)

    ids = jnp.full((2, half), -1, jnp.int32).at[:, :rows].set(verdict_ids.T).reshape(-1)
    vocab_rows = vocab_table.shape[0]
    local_ids = ids - jnp.where(ids >= 0, lax.axis_index("tp") * vocab_rows, 0)
    inside = (local_ids >= 0) & (local_ids < vocab_rows)
    table = vocab_table[jnp.clip(local_ids, 0, vocab_rows - 1)]
    table = jnp.where(inside[:, None], table, jnp.zeros_like(table))

    vmem = pl.BlockSpec(memory_space=pltpu.VMEM)
    smem = pl.BlockSpec(memory_space=pltpu.SMEM)
    peers_s, peers_t = max(ns - 1, 1), max(nt - 1, 1)
    dma = pltpu.SemaphoreType.DMA
    attended, hidden, win = pl.pallas_call(
        functools.partial(kernel, ns, nt, width, tuple(spans)),
        out_shape=(
            jax.ShapeDtypeStruct(q_prefill.shape, BF),
            jax.ShapeDtypeStruct(stream.shape, BF),
            jax.ShapeDtypeStruct((rows, 128), F32),
        ),
        in_specs=[smem, smem] + [vmem] * 9 + [pl.BlockSpec(memory_space=pl.ANY)],
        out_specs=(vmem, vmem, vmem),
        scratch_shapes=[
            pltpu.VMEM((slots, tokens, kv_width), BF),
            pltpu.VMEM((slots, tokens, kv_width), BF),
            pltpu.VMEM((tokens, tokens), F32),
            pltpu.VMEM((heads, tokens), F32),
            pltpu.VMEM((heads, tokens), F32),
            pltpu.VMEM((heads, HD, tokens), F32),
            pltpu.VMEM((ROW, heads * HD), F32),
            pltpu.VMEM((ROW, heads * HD), BF),
            pltpu.VMEM((ns, ROW, heads * HD), BF),
            pltpu.VMEM((HD, cols), BF),
            pltpu.VMEM((ROW, cols), F32),
            pltpu.VMEM((ns, HD, cols), BF),
            pltpu.VMEM((ns, ROW, cols), F32),
            pltpu.VMEM(out_weight.shape, BF),
            pltpu.VMEM((2 * ROW, columns), BF),
            pltpu.VMEM((nt, 2 * ROW, columns), BF),
            pltpu.VMEM((nt, 2 * half, columns), BF),
            pltpu.VMEM((rows, 128), F32),
            pltpu.VMEM((ns, rows, 128), F32),
            dma((slots,)), dma((slots,)), dma((slots,)), dma((slots,)),
            dma((peers_s,)), dma((peers_s,)),
            dma((peers_s,)), dma((peers_s,)),
            dma((peers_s,)), dma((peers_s,)),
            dma((peers_t,)), dma((peers_t,)),
            dma((peers_t,)), dma((peers_t,)),
            dma((peers_s,)), dma((peers_s,)),
            dma,
        ],
        compiler_params=pltpu.CompilerParams(
            collective_id=0, has_side_effects=True, vmem_limit_bytes=48 * 1024 * 1024
        ),
    )(
        pair_lengths, cache_lengths, q_prefill, k_prefill, v_prefill, q_decode, cache_k, cache_v,
        stream, norm_gain.reshape(1, columns), table, out_weight,
    )
    return attended, hidden, win[:, 0]


def solution(mesh):
    placed = (
        P(("groups", "seq"), "tp"),
        P(("groups", "seq"), "tp"),
        P(("groups", "seq"), "tp"),
        P("groups"),
        P("groups", "tp"),
        P("groups", "seq", "tp"),
        P("groups", "seq", "tp"),
        P("groups"),
        P("groups", "seq"),
        P("tp", "seq"),
        P("seq"),
        P("tp", "seq"),
        P("groups", None),
    )
    ns, nt = mesh.shape["seq"], mesh.shape["tp"]

    def body(*args):
        return shards(ns, nt, args[8].shape[1] * ns, *args)

    return jax.shard_map(
        body,
        mesh=mesh,
        in_specs=placed,
        out_specs=(P(("groups", "seq"), "tp"), P("groups", "seq"), P("groups")),
        check_vma=False,
    )
```

```python
import functools
import math

import jax
import jax.numpy as jnp
from jax import lax
from jax.experimental import pallas as pl
from jax.experimental.pallas import tpu as pltpu
from jax.sharding import PartitionSpec as P

HD = 128
ROW = 8
MASKED = -1e30
EPS = 1e-05
BF = jnp.bfloat16
F32 = jnp.float32
MESH = pl.DeviceIdType.MESH


def up(value, step):
    return -(-value // step) * step


def dot(a, b, dims):
    return lax.dot_general(a, b, (dims, ((), ())), preferred_element_type=F32)


def kernel(
    ns, nt, width, spans,
    len_in, clen_in, q_in, k_in, v_in, qd_in, ck_in, cv_in, stream_in, w_in, gain_ref, tbl_ref,
    att_ref, hid_ref, win_ref,
    len_ref, clen_ref, q_ref, k_ref, v_ref, qd_ref, ck_ref, cv_ref, stream_ref,
    kbuf, vbuf, bias, mrow, lrow, acc, qdpad, qsel, qx, pout, pstat, pox, psx, wbuf, part, partx, tblx, stat, statx,
    ks, kr, vs, vr, qs, qr, pos, por, pss, psr, ts, tr, gs, gr, ss, sr, loads,
):
    me = lax.axis_index("seq")
    mt = lax.axis_index("tp")
    tokens = q_ref.shape[0]
    heads = q_ref.shape[1] // HD
    kvl = k_ref.shape[1] // HD
    group = heads // kvl
    pairs = len_ref.shape[0]
    prompts, cache_n = ck_ref.shape[0], ck_ref.shape[1]
    scale2 = math.log2(math.e) / HD**0.5
    reach = len(spans)
    cols = pstat.shape[1]

    def head(h):
        return slice(h * HD, (h + 1) * HD)

    def relay(d, keys):
        src, buf, send, recv = (k_ref, kbuf, ks, kr) if keys else (v_ref, vbuf, vs, vr)
        low = spans[d - 1]
        rows = pl.ds(low, tokens - low)
        block = src.at[rows] if d == 1 else buf.at[d - 2, rows]
        return pltpu.make_async_remote_copy(
            src_ref=block,
            dst_ref=buf.at[d - 1, rows],
            send_sem=send.at[d - 1],
            recv_sem=recv.at[d - 1],
            device_id={"seq": lax.rem(me + 1, ns)},
            device_id_type=MESH,
        )

    def sends(d):
        return (me < ns - 1) & (me >= d - 1)

    def exchange(src, dst, send, recv, axis, mine, count):
        return [
            pltpu.make_async_remote_copy(
                src_ref=src,
                dst_ref=dst.at[mine],
                send_sem=send.at[d - 1],
                recv_sem=recv.at[d - 1],
                device_id={axis: lax.rem(mine + d, count)},
                device_id_type=MESH,
            )
            for d in range(1, count)
        ]

    places = (
        (k_in, k_ref), (len_in, len_ref), (q_in, q_ref), (v_in, v_ref), (clen_in, clen_ref),
        (qd_in, qd_ref), (ck_in, ck_ref), (cv_in, cv_ref), (stream_in, stream_ref), (w_in, wbuf),
    )
    fetches = [pltpu.make_async_copy(src, dst, loads.at[i]) for i, (src, dst) in enumerate(places)]
    for fetch in fetches:
        fetch.start()
    barrier = pltpu.get_barrier_semaphore()
    for d in range(1, ns):
        pl.semaphore_signal(barrier, inc=1, device_id={"seq": lax.rem(me + d, ns)}, device_id_type=MESH)
    for d in range(1, nt):
        pl.semaphore_signal(barrier, inc=1, device_id={"tp": lax.rem(mt + d, nt)}, device_id_type=MESH)

    fetches[0].wait()
    if ns + nt > 2:
        pl.semaphore_wait(barrier, ns + nt - 2)
    if reach:
        @pl.when(sends(1))
        def _():
            relay(1, True).start()
    for fetch in fetches[1:4]:
        fetch.wait()

    ends, total = [], jnp.int32(0)
    for p in range(pairs):
        total = total + len_ref[p]
        ends.append(total)
    starts = [jnp.int32(0)] + ends[:-1]
    first = me * tokens
    row_p = lax.broadcasted_iota(jnp.int32, (ROW, tokens), 0)
    last = jnp.full((ROW, tokens), -1, jnp.int32)
    for p in range(pairs):
        last = jnp.where(row_p == p, ends[p] - 1 - first, last)
    chosen = (lax.broadcasted_iota(jnp.int32, (ROW, tokens), 1) == last).astype(F32).astype(BF)
    picked = dot(chosen, q_ref[...], ((1,), (0,)))
    qsel[...] = picked.astype(BF)

    q_moves = exchange(qsel, qx, qs, qr, "seq", me, ns)
    for move in q_moves:
        move.start()
    if reach:
        @pl.when(sends(1))
        def _():
            relay(1, False).start()

    t_moves = exchange(tbl_ref, tblx, gs, gr, "tp", mt, nt)
    for move in t_moves:
        move.start()

    q_pos = lax.broadcasted_iota(jnp.int32, (tokens, tokens), 1)
    k_pos = lax.broadcasted_iota(jnp.int32, (tokens, tokens), 0)
    seg_start = jnp.zeros((1, tokens), jnp.int32)
    q_row = lax.broadcasted_iota(jnp.int32, (1, tokens), 1) + first
    for p in range(pairs):
        seg_start = jnp.where(ends[p] <= q_row, ends[p], seg_start)
    seg_local = seg_start - first

    def attend(d, low):
        count = tokens - low
        if d == 0:
            visible = (k_pos >= seg_local) & (k_pos <= q_pos)
        else:
            visible = k_pos[:count] + (low - d * tokens) >= seg_local
        bias[:count, :] = jnp.where(visible, 0.0, MASKED)
        for kv in range(kvl):
            if d == 0:
                keys, values = k_ref[:, head(kv)], v_ref[:, head(kv)]
            else:
                keys, values = kbuf[d - 1, low:, head(kv)], vbuf[d - 1, low:, head(kv)]
            values_t = values.T
            for g in range(group):
                h = kv * group + g
                s = dot(keys, q_ref[:, head(h)], ((1,), (1,))) + bias[:count, :]
                top = jnp.max(s, axis=0, keepdims=True)
                if d:
                    old = mrow[h : h + 1, :]
                    top = jnp.maximum(top, old)
                p = jnp.exp2((s - top) * scale2)
                weighted = dot(values_t, p.astype(BF), ((1,), (0,)))
                summed = jnp.sum(p, axis=0, keepdims=True)
                if d:
                    keep = jnp.exp2((old - top) * scale2)
                    summed = summed + lrow[h : h + 1, :] * keep
                    weighted = weighted + acc[h] * keep
                mrow[h : h + 1, :] = top
                lrow[h : h + 1, :] = summed
                acc[h] = weighted

    def step(d):
        @pl.when(me >= d)
        def _():
            relay(d, True).wait_recv()
            if d < reach:
                @pl.when(sends(d + 1))
                def _():
                    relay(d + 1, True).start()
            relay(d, False).wait_recv()
            if d < reach:
                @pl.when(sends(d + 1))
                def _():
                    relay(d + 1, False).start()
            attend(d, spans[d - 1])

    attend(0, 0)

    for fetch in fetches[4:8]:
        fetch.wait()
    for move in q_moves:
        move.wait_recv()
    q_pair = qsel[...].astype(F32)
    for d in range(1, ns):
        q_pair = q_pair + qx[lax.rem(me + d, ns)].astype(F32)
    qdpad[...] = jnp.zeros_like(qdpad)
    qdpad[:prompts, :] = qd_ref[...].astype(F32)
    q_dec = qdpad[...]
    pieces = [side[:, head(h)] for side in (q_pair, q_dec) for h in range(heads)]
    used = 2 * heads * ROW
    if cols > used:
        pieces.append(jnp.zeros((cols - used, HD), F32))
    q_cols = jnp.concatenate(pieces, axis=0).astype(BF)

    col = lax.broadcasted_iota(jnp.int32, (1, cols), 1)
    col_row = lax.rem(col, ROW)
    low_pair, high_pair = jnp.zeros((1, cols), jnp.int32), jnp.zeros((1, cols), jnp.int32)
    low_dec, high_dec = low_pair, high_pair
    for p in range(pairs):
        low_pair = jnp.where(col_row == p, starts[p] - first, low_pair)
        high_pair = jnp.where(col_row == p, ends[p] - first, high_pair)
    for p in range(prompts):
        ours = jnp.minimum(jnp.maximum(clen_ref[p] - me * cache_n, 0), cache_n)
        low_dec = jnp.where(col_row == p, p * cache_n, low_dec)
        high_dec = jnp.where(col_row == p, p * cache_n + ours, high_dec)

    blocks = []
    for kind in range(2):
        for kv in range(kvl):
            if kind == 0:
                keys, values = k_ref[:, head(kv)], v_ref[:, head(kv)]
                low_j, high_j = low_pair, high_pair
            else:
                keys = ck_ref[:, :, head(kv)].reshape(prompts * cache_n, HD)
                values = cv_ref[:, :, head(kv)].reshape(prompts * cache_n, HD)
                low_j, high_j = low_dec, high_dec
            begin = (kind * heads + kv * group) * ROW
            inside = (col >= begin) & (col < begin + group * ROW)
            high_j = jnp.where(inside, high_j, low_j)
            index = lax.broadcasted_iota(jnp.int32, (keys.shape[0], cols), 0)
            visible = (index >= low_j) & (index < high_j)
            s = jnp.where(visible, dot(keys, q_cols, ((1,), (1,))), MASKED)
            blocks.append((visible, s, values))
    top = functools.reduce(jnp.maximum, [jnp.max(s, axis=0, keepdims=True) for _, s, _ in blocks])
    p_sum = jnp.zeros((1, cols), F32)
    p_out = jnp.zeros((HD, cols), F32)
    for visible, s, values in blocks:
        p = jnp.where(visible, jnp.exp2((s - top) * scale2), 0.0)
        p_sum = p_sum + jnp.sum(p, axis=0, keepdims=True)
        p_out = p_out + dot(values.T, p.astype(BF), ((1,), (0,)))
    pout[...] = p_out.astype(BF)
    stat_row = lax.broadcasted_iota(jnp.int32, (ROW, cols), 0)
    pstat[...] = jnp.where(stat_row == 0, top, p_sum)
    o_moves = exchange(pout, pox, pos, por, "seq", me, ns)
    s_moves = exchange(pstat, psx, pss, psr, "seq", me, ns)
    for move, other in zip(o_moves, s_moves):
        move.start()
        other.start()
    pox[me] = pout[...]
    psx[me] = pstat[...]

    if reach:
        step(1)

    for move, other in zip(o_moves, s_moves):
        move.wait_recv()
        other.wait_recv()
    top = psx[0, 0:1, :]
    for i in range(1, ns):
        top = jnp.maximum(top, psx[i, 0:1, :])
    p_sum = jnp.zeros((1, cols), F32)
    p_out = jnp.zeros((HD, cols), F32)
    for i in range(ns):
        keep = jnp.exp2((psx[i, 0:1, :] - top) * scale2)
        p_sum = p_sum + psx[i, 1:2, :] * keep
        p_out = p_out + pox[i].astype(F32) * keep
    rows_t = (p_out / jnp.where(p_sum > 0.0, p_sum, 1.0)).T
    sides = [
        jnp.concatenate([rows_t[(kind * heads + h) * ROW : (kind * heads + h + 1) * ROW, :] for h in range(heads)], axis=1)
        for kind in range(2)
    ]
    verdict_in = jnp.concatenate(sides, axis=0).astype(BF)
    fetches[9].wait()
    part[...] = dot(verdict_in, wbuf[...], ((1,), (0,))).astype(BF)
    a_moves = exchange(part, partx, ts, tr, "tp", mt, nt)
    for move in a_moves:
        move.start()
    partx[mt] = part[...]
    tblx[mt] = tbl_ref[...]

    if reach > 1:
        step(2)

    for move in t_moves + a_moves:
        move.wait_recv()
    fetches[8].wait()
    rows = stream_ref.shape[0]
    table = tblx[0].astype(F32)
    added = partx[0].astype(F32)
    for i in range(1, nt):
        table = table + tblx[i].astype(F32)
        added = added + partx[i].astype(F32)
    half = table.shape[0] // 2
    residual = stream_ref[...].astype(F32) + jnp.concatenate([added[:pairs], added[ROW : ROW + prompts]], axis=0)
    gained = residual * gain_ref[...].astype(F32)
    squares = jnp.sum(residual * residual, axis=1, keepdims=True)
    raw0 = jnp.sum(gained * table[:rows], axis=1, keepdims=True)
    raw1 = jnp.sum(gained * table[half : half + rows], axis=1, keepdims=True)
    lane = lax.broadcasted_iota(jnp.int32, stat.shape, 1)
    stat[...] = jnp.where(lane == 0, squares, jnp.where(lane == 1, raw0, raw1))
    f_moves = exchange(stat, statx, ss, sr, "seq", me, ns)
    for move in f_moves:
        move.start()
    statx[me] = stat[...]

    for d in range(3, reach + 1):
        step(d)

    for h in range(heads):
        att_ref[:, head(h)] = (acc[h] / lrow[h : h + 1, :]).T.astype(BF)

    for move in f_moves:
        move.wait_recv()
    sums = statx[0]
    for i in range(1, ns):
        sums = sums + statx[i]
    inv = 1.0 / jnp.sqrt(sums[:, 0:1] / width + EPS)
    hid_ref[...] = (gained * inv).astype(BF)
    win = 1.0 / (1.0 + jnp.exp(sums[:, 2:3] * inv - sums[:, 1:2] * inv))
    win_ref[...] = jnp.broadcast_to(win, win_ref.shape)

    for d in range(1, reach + 1):
        @pl.when(sends(d))
        def _():
            relay(d, True).wait_send()
            relay(d, False).wait_send()
    for move in q_moves + t_moves + o_moves + s_moves + a_moves + f_moves:
        move.wait_send()


def lookup(ids_in, table_in, out_ref, ids_ref, stage, lines, ids_sem, sems):
    vocab_rows = table_in.shape[0]
    fetch = pltpu.make_async_copy(ids_in, ids_ref, ids_sem)
    fetch.start()
    base = lax.axis_index("tp") * vocab_rows
    lines[...] = jnp.zeros_like(lines)
    fetch.wait()
    sides, rows = ids_ref.shape
    half = out_ref.shape[0] // sides
    moves = []
    for c in range(sides):
        for r in range(rows):
            local = ids_ref[c, r] - base
            own = (local >= 0) & (local < vocab_rows)
            local = jnp.where(own, local, 0)
            spot = local & (ROW - 1)
            top = pl.multiple_of(local - spot, ROW)
            slot = c * rows + r
            move = pltpu.make_async_copy(table_in.at[pl.ds(top, ROW), :], stage.at[slot], sems.at[slot])
            move.start()
            moves.append((move, slot, c * half + r, jnp.where(own, spot, -1)))
    line = lax.broadcasted_iota(jnp.int32, stage.shape[1:], 0)
    for move, slot, at, spot in moves:
        move.wait()
        kept = jnp.where(line == spot, stage[slot].astype(F32), 0.0)
        lines[at : at + 1, :] = jnp.sum(kept, axis=0, keepdims=True)
    out_ref[...] = lines[...].astype(BF)


def shards(
    ns, nt, width,
    q_prefill, k_prefill, v_prefill, pair_lengths, q_decode, cache_k, cache_v, cache_lengths,
    stream, out_weight, norm_gain, vocab_table, verdict_ids,
):
    tokens, kv_width = k_prefill.shape
    heads = q_prefill.shape[1] // HD
    rows, columns = stream.shape
    most = tokens * ns * 5 // 8
    spans = []
    for d in range(1, ns):
        low = max(0, d * tokens - most + 1)
        if low < tokens:
            spans.append(low // 128 * 128)
    reach = len(spans)
    slots = max(reach, 1)
    cols = up(2 * heads * ROW, 128)
    half = up(rows, 16)

    vmem = pl.BlockSpec(memory_space=pltpu.VMEM)
    peers_s, peers_t = max(ns - 1, 1), max(nt - 1, 1)
    dma = pltpu.SemaphoreType.DMA
    hbm = pl.BlockSpec(memory_space=pltpu.HBM)
    table = pl.pallas_call(
        lookup,
        out_shape=jax.ShapeDtypeStruct((2 * half, columns), BF),
        in_specs=[hbm, hbm],
        out_specs=vmem,
        scratch_shapes=[
            pltpu.SMEM((2, rows), jnp.int32),
            pltpu.VMEM((2 * rows, ROW, columns), BF),
            pltpu.VMEM((2 * half, columns), F32),
            dma,
            dma((2 * rows,)),
        ],
        compiler_params=pltpu.CompilerParams(vmem_limit_bytes=8 * 1024 * 1024),
    )(verdict_ids.T, vocab_table)
    attended, hidden, win = pl.pallas_call(
        functools.partial(kernel, ns, nt, width, tuple(spans)),
        out_shape=(
            jax.ShapeDtypeStruct(q_prefill.shape, BF),
            jax.ShapeDtypeStruct(stream.shape, BF),
            jax.ShapeDtypeStruct((rows, 128), F32),
        ),
        in_specs=[hbm] * 10 + [vmem, vmem],
        out_specs=(vmem, vmem, vmem),
        scratch_shapes=[
            pltpu.SMEM(pair_lengths.shape, jnp.int32),
            pltpu.SMEM(cache_lengths.shape, jnp.int32),
            pltpu.VMEM(q_prefill.shape, BF),
            pltpu.VMEM(k_prefill.shape, BF),
            pltpu.VMEM(v_prefill.shape, BF),
            pltpu.VMEM(q_decode.shape, BF),
            pltpu.VMEM(cache_k.shape, BF),
            pltpu.VMEM(cache_v.shape, BF),
            pltpu.VMEM(stream.shape, BF),
            pltpu.VMEM((slots, tokens, kv_width), BF),
            pltpu.VMEM((slots, tokens, kv_width), BF),
            pltpu.VMEM((tokens, tokens), F32),
            pltpu.VMEM((heads, tokens), F32),
            pltpu.VMEM((heads, tokens), F32),
            pltpu.VMEM((heads, HD, tokens), F32),
            pltpu.VMEM((ROW, heads * HD), F32),
            pltpu.VMEM((ROW, heads * HD), BF),
            pltpu.VMEM((ns, ROW, heads * HD), BF),
            pltpu.VMEM((HD, cols), BF),
            pltpu.VMEM((ROW, cols), F32),
            pltpu.VMEM((ns, HD, cols), BF),
            pltpu.VMEM((ns, ROW, cols), F32),
            pltpu.VMEM(out_weight.shape, BF),
            pltpu.VMEM((2 * ROW, columns), BF),
            pltpu.VMEM((nt, 2 * ROW, columns), BF),
            pltpu.VMEM((nt, 2 * half, columns), BF),
            pltpu.VMEM((rows, 128), F32),
            pltpu.VMEM((ns, rows, 128), F32),
            dma((slots,)), dma((slots,)), dma((slots,)), dma((slots,)),
            dma((peers_s,)), dma((peers_s,)),
            dma((peers_s,)), dma((peers_s,)),
            dma((peers_s,)), dma((peers_s,)),
            dma((peers_t,)), dma((peers_t,)),
            dma((peers_t,)), dma((peers_t,)),
            dma((peers_s,)), dma((peers_s,)),
            dma((10,)),
        ],
        compiler_params=pltpu.CompilerParams(
            collective_id=0, has_side_effects=True, vmem_limit_bytes=48 * 1024 * 1024
        ),
    )(
        pair_lengths, cache_lengths, q_prefill, k_prefill, v_prefill, q_decode, cache_k, cache_v,
        stream, out_weight, norm_gain.reshape(1, columns), table,
    )
    return attended, hidden, win[:, 0]


def solution(mesh):
    placed = (
        P(("groups", "seq"), "tp"),
        P(("groups", "seq"), "tp"),
        P(("groups", "seq"), "tp"),
        P("groups"),
        P("groups", "tp"),
        P("groups", "seq", "tp"),
        P("groups", "seq", "tp"),
        P("groups"),
        P("groups", "seq"),
        P("tp", "seq"),
        P("seq"),
        P("tp", "seq"),
        P("groups", None),
    )
    ns, nt = mesh.shape["seq"], mesh.shape["tp"]

    def body(*args):
        return shards(ns, nt, args[8].shape[1] * ns, *args)

    return jax.shard_map(
        body,
        mesh=mesh,
        in_specs=placed,
        out_specs=(P(("groups", "seq"), "tp"), P("groups", "seq"), P("groups")),
        check_vma=False,
    )
```
